32 devices in a mesh: dp: 8 (over z, core), tensor: 4 (over y, x).
Axes of the slice: x: 2, y: 2, z: 4, core: 2. Of those that a mesh axis runs over, the one named last changes fastest.
Arguments:
- block_input: bfloat16 [2048, 5120], P('dp'), may hold values from -6 to 6
- query_weight: bfloat16 [2560, 5120], P('tensor'), as said below
- query_gain: float32 [2560], P('tensor'), may hold values from 0.5 to 2
- query_grad: bfloat16 [2560, 2048], P('tensor', 'dp'), may hold values from -6 to 6
Outputs:
- input_grad: bfloat16 [2048, 5120], P(('dp', 'tensor'))
- weight_grad: float32 [5120, 2560], P('dp', 'tensor')
The draws below stay inside these ranges and needn't reach their ends.
Inputs may be any that keep to these rules, and one draw needn't show every extreme that they name: `query_weight`: entries are normal with standard deviation 5120 ** -0.5 times a factor between 0.25 and 75, which may differ from row to row and from column to column.
All inputs are finite; a program needn't handle non-finite values.
Results may differ from the reference program's by a relative error of at most 0.017.
Values may be sent and summed in bfloat16 or wider, within the bound.
No kernel may reach another device: no remote copies, remote signals or barrier semaphores. Data moves between devices by JAX's collectives and lax.ppermute only.
A program may use at most 64 MiB of HBM per device.

```python
import math
import jax
import jax.numpy as jnp
from jax import lax

D = 5120
HQ = 2560
TOKENS = 2048
N_TENSOR = 4


def draw_query_weight(key, part):
    first = jax.random.fold_in(key, 0)
    base = jax.random.normal(first, (HQ, D), jnp.float32) / math.sqrt(D)
    ramp = jnp.exp(math.log(3.0) * jnp.arange(HQ, dtype=jnp.float32) / HQ)[:, None]
    return (base * ramp).astype(jnp.bfloat16)


def strengthened(values, stream_key, source, target, shards_of, factor):
    def block_of(dim):
        return (jnp.arange(values.shape[dim]) // (values.shape[dim] // shards_of)).reshape((-1,) + (1,) * (values.ndim - 1 - dim))

    first = jax.random.permutation(stream_key, shards_of)[block_of(target)]
    far = (block_of(target) + shards_of // 2) % shards_of
    return jnp.where((block_of(source) == first) | (block_of(source) == far), factor * values, values)


def block_levels(rng, extent, shards, least, high):
    factor_of, own = 1.0, jax.random.fold_in(rng, 6)
    for position, parts in shards:
        steps = jnp.exp(jax.random.uniform(jax.random.fold_in(own, position), (parts,), jnp.float32, least / len(shards), high / len(shards)))
        factor_of = factor_of * jnp.repeat(steps, extent[position] // parts).reshape([-1 if axis == position else 1 for axis in range(len(extent))])
    return factor_of


def centred(key, shape, deviation, limit, cuts=(), held_as=jnp.bfloat16):
    factor_of = block_levels(key, shape, cuts, -0.22, 0.18) if cuts else 1.0
    result = jax.random.normal(key, shape, jnp.float32) * deviation * factor_of
    return jnp.minimum(jnp.maximum(result, -limit), limit).astype(held_as)


def heavy_noise(stream_key, dims, scale, most, cuts, heavy, kind=jnp.bfloat16):
    values = scale * jax.random.normal(stream_key, dims, jnp.float32)
    if cuts:
        values = values * block_levels(stream_key, dims, cuts, -0.22, 0.18)
    return jnp.clip(strengthened(values, jax.random.fold_in(stream_key, 3), *heavy), -most, most).astype(kind)


def setup_inputs(seed: int = 0) -> dict:
    splits = jax.random.split(jax.random.key(seed), 5)
    return {
        "block_input": heavy_noise(splits[0], (TOKENS, D), 1.0, 6.0, ((0, 8),), (0, 1, 8, 2.0)),
        "query_weight": draw_query_weight(jax.random.fold_in(splits[4], 71), 0),
        "query_gain": jnp.clip(jnp.exp(math.log(2.0) - 1.3862944 * jax.random.uniform(splits[2], (HQ,), jnp.float32) ** block_levels(splits[2], (HQ,), ((0, 4),), -0.2, 0.2)), 0.5, 2.0),
        "query_grad": centred(splits[3], (HQ, TOKENS), 1.0, 6.0, ((0, 4), (1, 8))),
    }


epsilon = 1e-06

def reference(block_input, query_weight, query_gain, query_grad):
    projected = jnp.dot(block_input, query_weight.T, preferred_element_type=jnp.float32)
    squares = lax.optimization_barrier(jnp.sum(projected * projected, axis=1, keepdims=True))
    inverse_rms = 1.0 / jnp.sqrt(squares / HQ + epsilon)
    scaled_grad = query_grad.T.astype(jnp.float32) * query_gain
    cross_sums = lax.optimization_barrier(jnp.sum(scaled_grad * projected, axis=1, keepdims=True))
    coefficient = inverse_rms * inverse_rms * inverse_rms * (cross_sums / HQ)
    proj_grad = (inverse_rms * scaled_grad - coefficient * projected).astype(jnp.bfloat16)
    group = HQ // N_TENSOR
    total = jnp.zeros((TOKENS, D), jnp.float32)
    for member in range(N_TENSOR):
        lower = member * group
        term = jnp.dot(proj_grad[:, lower:lower + group], query_weight[lower:lower + group, :], preferred_element_type=jnp.float32)
        rounded = lax.optimization_barrier(term.astype(jnp.bfloat16)).astype(jnp.float32)
        total = total + rounded
    input_grad = total.astype(jnp.bfloat16)
    weight_grad = jnp.dot(block_input.T, proj_grad, preferred_element_type=jnp.float32)
    return (input_grad, weight_grad)
```

```python
import jax
import jax.numpy as jnp
from jax import lax
from jax.sharding import PartitionSpec as P

epsilon = 1e-06


def partner(index, step):
    return index ^ step


def exchange(value, axis, pairs):
    return lax.ppermute(value, axis, pairs)


def make(mesh):
    dp, members = mesh.shape["dp"], mesh.shape["tensor"]
    cores = 2 if dp % 2 == 0 else 1
    planes = dp // cores

    def tensor_pairs(step):
        return [(i, partner(i, step)) for i in range(members)]

    def plane_pairs(step):
        return [
            (p * cores + c, partner(p, step) * cores + c)
            for p in range(planes)
            for c in range(cores)
        ]

    def per_device(block_input, query_weight, query_gain, query_grad):
        tokens, width = block_input.shape
        features = query_gain.shape[0]
        part = tokens // members
        columns = width // planes
        group = lax.axis_index("dp")
        plane, core = group // cores, group % cores
        me = lax.axis_index("tensor")

        arrived = []
        for s in range(1, planes):
            piece = lax.dynamic_slice(
                block_input, (me * part, partner(plane, s) * columns), (part, columns)
            )
            arrived.append(exchange(piece, "dp", plane_pairs(s)))
        arrived = jnp.stack(arrived)

        projected = lax.dot_general(
            block_input, query_weight, (((1,), (1,)), ((), ())), preferred_element_type=jnp.float32
        )
        scaled_grad = query_grad.T.astype(jnp.float32) * query_gain[None, :]
        sums = jnp.stack(
            [jnp.sum(projected * projected, axis=1), jnp.sum(scaled_grad * projected, axis=1)]
        )
        total = sums
        for r in range(1, members):
            total = total + exchange(sums, "tensor", tensor_pairs(r))
        squares, cross_sums = total[0], total[1]
        count = features * members
        inverse_rms = 1.0 / jnp.sqrt(squares / count + epsilon)
        coefficient = inverse_rms * inverse_rms * inverse_rms * (cross_sums / count)
        proj_grad = (
            inverse_rms[:, None] * scaled_grad - coefficient[:, None] * projected
        ).astype(jnp.bfloat16)
        proj_grad = jnp.concatenate(
            [
                lax.dynamic_slice_in_dim(proj_grad, partner(me, r) * part, part, 0)
                for r in range(members)
            ]
        )
        grads = [proj_grad] + [exchange(proj_grad, "dp", plane_pairs(s)) for s in range(1, planes)]

        partial = lax.dot_general(
            proj_grad, query_weight, (((1,), (0,)), ((), ())), preferred_element_type=jnp.float32
        ).astype(jnp.bfloat16)
        summed = partial[:part].astype(jnp.float32)
        for r in range(1, members):
            summed = summed + exchange(
                partial[r * part : (r + 1) * part], "tensor", tensor_pairs(r)
            ).astype(jnp.float32)
        input_grad = summed.astype(jnp.bfloat16)

        shared = [arrived] + [exchange(arrived, "tensor", tensor_pairs(r)) for r in range(1, members)]
        own = [
            lax.dynamic_slice(
                block_input, (partner(me, r) * part, plane * columns), (part, columns)
            )
            for r in range(members)
        ]
        inputs = own + [shared[r][s] for s in range(planes - 1) for r in range(members)]
        weight = lax.dot_general(
            jnp.concatenate(inputs),
            jnp.concatenate(grads),
            (((0,), (0,)), ((), ())),
            preferred_element_type=jnp.float32,
        )
        rows = columns // cores
        kept = lax.dynamic_slice_in_dim(weight, core * rows, rows, 0)
        if cores == 2:
            given = lax.dynamic_slice_in_dim(weight, (1 - core) * rows, rows, 0)
            swap = [(i, i ^ 1) for i in range(dp)]
            kept = kept + exchange(given, "dp", swap)
        return (input_grad, kept)

    return per_device


def solution(mesh):
    in_specs = (P("dp", None), P("tensor", None), P("tensor"), P("tensor", "dp"))
    out_specs = (P(("dp", "tensor"), None), P("dp", "tensor"))
    return jax.shard_map(
        make(mesh), mesh=mesh, in_specs=in_specs, out_specs=out_specs, check_vma=False
    )
```

```python
import jax
import jax.numpy as jnp
from jax import lax
from jax.experimental import pallas as pl
from jax.experimental.pallas import tpu as pltpu
from jax.sharding import PartitionSpec as P


epsilon = 1e-06
f32, bf16 = jnp.float32, jnp.bfloat16
WHOLE = pl.BlockSpec(memory_space=pltpu.VMEM)


def dot(a, b, ca, cb):
    return lax.dot_general(a, b, (((ca,), (cb,)), ((), ())), preferred_element_type=f32)


def cost(flops, nbytes):
    return pl.CostEstimate(flops=flops, bytes_accessed=nbytes, transcendentals=0)


def sds(shape, dtype):
    return jax.ShapeDtypeStruct(shape, dtype)


def chunk(size, most):
    fits = [c for c in range(128, most + 1, 128) if size % c == 0]
    return fits[-1] if fits else size


def params(nbytes):
    return pltpu.CompilerParams(vmem_limit_bytes=max(nbytes, 4 << 20))


def pick(block_input, columns, part, counts, cores):
    tokens = block_input.shape[0]
    shapes = [(part if mine else tokens, columns) for _, mine in counts]

    def place(step, mine):
        plane, me = lax.axis_index("dp") // cores, lax.axis_index("tensor")
        return (me * part if mine else 0), (plane ^ step) * columns

    def kernel(x_ref, *outs):
        for out, (step, mine) in zip(outs, counts):
            row, column = place(step, mine)
            rows = pl.ds(pl.multiple_of(row, part), out.shape[0])
            out[...] = x_ref[rows, pl.ds(pl.multiple_of(column, columns), columns)]

    if columns % 128:
        return [lax.dynamic_slice(block_input, place(*c), shape) for c, shape in zip(counts, shapes)]
    return pl.pallas_call(
        kernel,
        in_specs=[WHOLE],
        out_specs=[WHOLE] * len(shapes),
        out_shape=[sds(shape, bf16) for shape in shapes],
        cost_estimate=cost(1, 4 * sum(r * c for r, c in shapes)),
        compiler_params=params(2 << 20),
        name="pick",
    )(block_input)


def column(row, size):
    return jnp.broadcast_to(row, (128, size)).T[:, :1]


def project(block_input, query_weight, query_grad, gain):
    tokens, width = block_input.shape
    features = query_weight.shape[0]
    wide = chunk(width, 2560)

    def kernel(x_ref, w_ref, g_ref, gain_ref, out_ref, sums_ref):
        for k in range(0, width, wide):
            product = dot(w_ref[:, k : k + wide], x_ref[:, k : k + wide], 1, 1)
            out_ref[...] = product if k == 0 else out_ref[...] + product
        projected = out_ref[...]
        scaled = g_ref[...].astype(f32) * column(gain_ref[...], features)
        sums_ref[0:1, :] = jnp.sum(projected * projected, axis=0, keepdims=True)
        sums_ref[1:2, :] = jnp.sum(scaled * projected, axis=0, keepdims=True)

    return pl.pallas_call(
        kernel,
        in_specs=[WHOLE] * 4,
        out_specs=[WHOLE] * 2,
        out_shape=[sds((features, tokens), f32), sds((2, tokens), f32)],
        cost_estimate=cost(2 * tokens * features * width, 2 * width * (tokens + features)),
        compiler_params=params(16 << 20),
        name="project",
    )(block_input, query_weight, query_grad, gain)


def backward(projected, query_grad, gain, first, second, members):
    features, tokens = projected.shape
    part = tokens // members

    def kernel(p_ref, g_ref, gain_ref, first_ref, second_ref, out_ref):
        total = (first_ref[...] + second_ref[...]) / (features * members)
        inverse_rms = 1.0 / jnp.sqrt(total[0:1] + epsilon)
        coefficient = inverse_rms * inverse_rms * inverse_rms * total[1:2]
        scaled = g_ref[...].astype(f32) * column(gain_ref[...], features)
        grad = (inverse_rms * scaled - coefficient * p_ref[...]).T.astype(bf16)
        me = lax.axis_index("tensor")
        for q in range(members):
            rows = pl.ds(pl.multiple_of((me ^ q) * part, part), part)
            out_ref[rows, :] = grad[q * part : (q + 1) * part]

    return pl.pallas_call(
        kernel,
        in_specs=[WHOLE] * 5,
        out_specs=WHOLE,
        out_shape=sds((tokens, features), bf16),
        cost_estimate=cost(6 * features * tokens, 8 * features * tokens),
        compiler_params=params(6 << 20),
        name="backward",
    )(projected, query_grad, gain, first, second)


def spread(proj_grad, query_weight, members):
    tokens, features = proj_grad.shape
    width = query_weight.shape[1]
    part = tokens // members
    wide = chunk(width, 1280)

    def kernel(p_ref, w_ref, *outs):
        for k in range(0, width, wide):
            product = dot(p_ref[...], w_ref[:, k : k + wide], 1, 0).astype(bf16)
            for r in range(members):
                outs[r][:, k : k + wide] = product[r * part : (r + 1) * part]

    return pl.pallas_call(
        kernel,
        in_specs=[WHOLE] * 2,
        out_specs=[WHOLE] * members,
        out_shape=[sds((part, width), bf16)] * members,
        cost_estimate=cost(2 * tokens * features * width, 2 * width * (tokens + features)),
        compiler_params=params(8 << 20),
        name="spread",
    )(proj_grad, query_weight)


def total_of(pieces):
    part, width = pieces[0].shape

    def kernel(*refs):
        refs[-1][...] = sum(ref[...].astype(f32) for ref in refs[:-1]).astype(bf16)

    return pl.pallas_call(
        kernel,
        in_specs=[WHOLE] * len(pieces),
        out_specs=WHOLE,
        out_shape=sds((part, width), bf16),
        cost_estimate=cost(4 * part * width, 10 * part * width),
        compiler_params=params(6 << 20),
        name="total",
    )(*pieces)


def weight_product(own, terms, grads, rows, cores, extra=None):
    arrays = []
    for t in terms:
        if not any(t[0] is a for a in arrays):
            arrays.append(t[0])
    places = [next(i for i, a in enumerate(arrays) if a is t[0]) for t in terms]
    features = grads[0].shape[1]
    depth = sum(t[2] for t in terms)
    span = rows * cores if own is None else rows

    def first_column(core, start):
        if own is None:
            return start
        return start + (core if own else 1 - core) * rows

    def first_row(row, slot, part):
        return row if slot is None else (lax.axis_index("tensor") ^ slot) * part

    def kernel(*refs):
        core, plane = lax.axis_index("dp") % cores, lax.axis_index("dp") // cores
        xs, gs = refs[: len(arrays)], refs[len(arrays) : len(arrays) + len(grads)]
        out_ref, x_all, g_all = refs[-3], refs[-2], refs[-1]
        done = 0
        for place, (_, row, count, g, start, slot, planed) in zip(places, terms):
            offset = first_column(core, plane * rows * cores if planed else 0)
            cols = pl.ds(pl.multiple_of(offset, rows), span)
            begin = first_row(row, slot, count)
            x_all[done : done + count] = xs[place][pl.ds(pl.multiple_of(begin, count), count), cols]
            g_all[done : done + count] = gs[g][start : start + count]
            done += count
        value = dot(x_all[...], g_all[...], 0, 0)
        if extra is None:
            out_ref[...] = value
        else:
            half = pl.ds(pl.multiple_of(first_column(core, 0), rows), span)
            out_ref[...] = value + refs[-4][half, :]

    if rows % 128:
        core, plane = lax.axis_index("dp") % cores, lax.axis_index("dp") // cores
        xs = [
            lax.dynamic_slice(
                t[0],
                (
                    first_row(t[1], t[5], t[2]),
                    first_column(core, plane * rows * cores if t[6] else 0),
                ),
                (t[2], span),
            )
            for t in terms
        ]
        gs = [grads[t[3]][t[4] : t[4] + t[2]] for t in terms]
        value = dot(jnp.concatenate(xs), jnp.concatenate(gs), 0, 0)
        if extra is None:
            return value
        return value + lax.dynamic_slice_in_dim(extra, first_column(core, 0), span, 0)
    operands = arrays + list(grads) + ([] if extra is None else [extra])
    return pl.pallas_call(
        kernel,
        in_specs=[WHOLE] * len(operands),
        out_specs=WHOLE,
        out_shape=sds((span, features), f32),
        scratch_shapes=[pltpu.VMEM((depth, span), bf16), pltpu.VMEM((depth, features), bf16)],
        cost_estimate=cost(2 * span * features * depth, 4 * span * features),
        compiler_params=params(16 << 20),
        name="weight_product",
    )(*operands)


def make(mesh):
    dp, members = mesh.shape["dp"], mesh.shape["tensor"]
    cores = 2
    planes = dp // cores
    if dp % cores or planes & (planes - 1) or members & (members - 1):
        raise ValueError("sizes")

    def across(value, step):
        return lax.ppermute(value, "tensor", [(i, i ^ step) for i in range(members)])

    def along(value, step):
        pairs = [(i, i ^ (step * cores)) for i in range(dp)]
        return lax.ppermute(value, "dp", pairs)

    def per_device(block_input, query_weight, query_gain, query_grad):
        tokens, width = block_input.shape
        features = query_gain.shape[0]
        part = tokens // members
        columns = width // planes
        rows = columns // cores
        gain = query_gain.reshape(1, features)

        counts = [(s, s > 1) for s in range(planes - 1, 0, -1)]
        blocks = pick(block_input, columns, part, counts, cores)
        inputs = {s: along(block, s) for (s, _), block in zip(counts, blocks)}

        projected, sums = project(block_input, query_weight, query_grad, gain)
        step = 1
        while step < members // 2:
            sums = sums + across(sums, step)
            step *= 2
        other = across(sums, step) if members > 1 else jnp.zeros_like(sums)
        proj_grad = backward(projected, query_grad, gain, sums, other, members)
        grads = {s: along(proj_grad, s) for s in range(1, planes)}

        pieces = spread(proj_grad, query_weight, members)
        pieces = [pieces[0]] + [across(pieces[r], r) for r in range(1, members)]
        input_grad = total_of(pieces)

        early = [(block_input, 0, part, 0, r * part, r, True) for r in range(members)]
        begun = weight_product(None, early, [proj_grad], rows, cores)
        late, order = [], list(grads)
        if planes > 1:
            late += [(inputs[1], 0, part, 0, r * part, r, False) for r in range(members)]
        far = order[1:]
        late += [(inputs[s], 0, part, order.index(s), 0, None, False) for s in far]
        if far and members > 1:
            joined = jnp.concatenate([inputs[s] for s in far])
            for r in range(1, members):
                array = across(joined, r)
                late += [
                    (array, k * part, part, order.index(s), r * part, None, False)
                    for k, s in enumerate(far)
                ]
        late_grads = [grads[s] for s in order]
        given = weight_product(0, late, late_grads, rows, cores, begun)
        given = lax.ppermute(given, "dp", [(i, i ^ 1) for i in range(dp)])
        kept = weight_product(1, late, late_grads, rows, cores, begun)
        weight_grad = kept + given
        return (input_grad, weight_grad)

    return per_device


def solution(mesh):
    in_specs = (P("dp", None), P("tensor", None), P("tensor"), P("tensor", "dp"))
    out_specs = (P(("dp", "tensor"), None), P("dp", "tensor"))
    return jax.shard_map(
        make(mesh), mesh=mesh, in_specs=in_specs, out_specs=out_specs, check_vma=False
    )
```

```python
import jax
import jax.numpy as jnp
from jax import lax
from jax.experimental import pallas as pl
from jax.experimental.pallas import tpu as pltpu
from jax.sharding import PartitionSpec as P


epsilon = 1e-06
f32, bf16 = jnp.float32, jnp.bfloat16
WHOLE = pl.BlockSpec(memory_space=pltpu.VMEM)


def dot(a, b, ca, cb):
    return lax.dot_general(a, b, (((ca,), (cb,)), ((), ())), preferred_element_type=f32)


def cost(flops, nbytes):
    return pl.CostEstimate(flops=flops, bytes_accessed=nbytes, transcendentals=0)


def sds(shape, dtype):
    return jax.ShapeDtypeStruct(shape, dtype)


def chunk(size, most):
    fits = [c for c in range(128, most + 1, 128) if size % c == 0]
    return fits[-1] if fits else size


def params(nbytes):
    return pltpu.CompilerParams(vmem_limit_bytes=max(nbytes, 4 << 20))


def stage(block_input, query_weight, query_grad, columns, part, counts, cores):
    tokens = block_input.shape[0]
    operands = [block_input, query_weight, query_grad]
    shapes = [(tokens if slots is None else part * len(slots), columns) for _, slots in counts]

    def places(step, slots):
        plane, me = lax.axis_index("dp") // cores, lax.axis_index("tensor")
        rows = [(0, tokens)] if slots is None else [((me ^ r) * part, part) for r in slots]
        return [(row, count, (plane ^ step) * columns) for row, count in rows]

    if columns % 128:
        return operands, [
            jnp.concatenate(
                [lax.dynamic_slice(block_input, (p[0], p[2]), (p[1], columns)) for p in places(*c)]
            )
            for c in counts
        ]

    def kernel(*refs):
        ins, held, outs, sem = refs[:3], refs[3:6], refs[6:-1], refs[-1]
        copies = [pltpu.make_async_copy(i, h, sem.at[n]) for n, (i, h) in enumerate(zip(ins, held))]
        for copy in copies:
            copy.start()
        copies[0].wait()
        for out, entry in zip(outs, counts):
            done = 0
            for row, count, column in places(*entry):
                rows = pl.ds(pl.multiple_of(row, part), count)
                out[done : done + count] = held[0][rows, pl.ds(pl.multiple_of(column, columns), columns)]
                done += count
        for copy in copies[1:]:
            copy.wait()

    results = pl.pallas_call(
        kernel,
        in_specs=[pl.BlockSpec(memory_space=pl.ANY)] * 3,
        out_specs=[WHOLE] * (3 + len(shapes)),
        out_shape=[pltpu.VMEM(o.shape, o.dtype) for o in operands]
        + [pltpu.VMEM(shape, bf16) for shape in shapes],
        scratch_shapes=[pltpu.SemaphoreType.DMA((3,))],
        cost_estimate=cost(1, 4 * sum(r * c for r, c in shapes)),
        compiler_params=params(2 << 20),
        name="stage",
    )(*[pltpu.with_memory_space_constraint(o, pltpu.HBM) for o in operands])
    return results[:3], results[3:]


def column(row, size):
    return jnp.broadcast_to(row, (128, size)).T[:, :1]


def project(block_input, query_weight, query_grad, gain):
    tokens, width = block_input.shape
    features = query_weight.shape[0]
    wide = chunk(width, 2560)

    def kernel(x_ref, w_ref, g_ref, gain_ref, out_ref, sums_ref):
        for k in range(0, width, wide):
            product = dot(w_ref[:, k : k + wide], x_ref[:, k : k + wide], 1, 1)
            out_ref[...] = product if k == 0 else out_ref[...] + product
        projected = out_ref[...]
        scaled = g_ref[...].astype(f32) * column(gain_ref[...], features)
        sums_ref[0:1, :] = jnp.sum(projected * projected, axis=0, keepdims=True)
        sums_ref[1:2, :] = jnp.sum(scaled * projected, axis=0, keepdims=True)

    return pl.pallas_call(
        kernel,
        in_specs=[WHOLE] * 4,
        out_specs=[WHOLE] * 2,
        out_shape=[pltpu.VMEM((features, tokens), f32), pltpu.VMEM((2, tokens), f32)],
        cost_estimate=cost(2 * tokens * features * width, 2 * width * (tokens + features)),
        compiler_params=params(16 << 20),
        name="project",
    )(block_input, query_weight, query_grad, gain)


def backward(projected, query_grad, gain, sums, members):
    features, tokens = projected.shape
    part = tokens // members

    def kernel(p_ref, g_ref, gain_ref, *refs):
        *sums_refs, out_ref = refs
        total = sum(ref[...] for ref in sums_refs) / (features * members)
        inverse_rms = 1.0 / jnp.sqrt(total[0:1] + epsilon)
        coefficient = inverse_rms * inverse_rms * inverse_rms * total[1:2]
        scaled = g_ref[...].astype(f32) * column(gain_ref[...], features)
        grad = (inverse_rms * scaled - coefficient * p_ref[...]).T.astype(bf16)
        me = lax.axis_index("tensor")
        for q in range(members):
            rows = pl.ds(pl.multiple_of((me ^ q) * part, part), part)
            out_ref[rows, :] = grad[q * part : (q + 1) * part]

    return pl.pallas_call(
        kernel,
        in_specs=[WHOLE] * (3 + len(sums)),
        out_specs=WHOLE,
        out_shape=pltpu.VMEM((tokens, features), bf16),
        cost_estimate=cost(6 * features * tokens, 8 * features * tokens),
        compiler_params=params(6 << 20),
        name="backward",
    )(projected, query_grad, gain, *sums)


def spread(proj_grad, query_weight, members):
    tokens, features = proj_grad.shape
    width = query_weight.shape[1]
    part = tokens // members
    wide = chunk(width, 1280)

    def kernel(p_ref, w_ref, *outs):
        for k in range(0, width, wide):
            product = dot(p_ref[...], w_ref[:, k : k + wide], 1, 0).astype(bf16)
            for r in range(members):
                outs[r][:, k : k + wide] = product[r * part : (r + 1) * part]

    return pl.pallas_call(
        kernel,
        in_specs=[WHOLE] * 2,
        out_specs=[WHOLE] * members,
        out_shape=[sds((part, width), bf16)] * members,
        cost_estimate=cost(2 * tokens * features * width, 2 * width * (tokens + features)),
        compiler_params=params(8 << 20),
        name="spread",
    )(proj_grad, query_weight)


def spread_half(proj_grad, query_weight, color, part):
    tokens, features = proj_grad.shape
    half = query_weight.shape[1] // 2
    first, second = (1, 2) if color == 0 else (2, 1)
    wide = chunk(half, 1280)

    def kernel(p_ref, w_ref, send_ref, own_ref, pass_ref):
        for k in range(0, half, wide):
            here = slice(color * half + k, color * half + k + wide)
            product = dot(p_ref[...], w_ref[:, here], 1, 0).astype(bf16)
            slot = [product[r * part : (r + 1) * part] for r in range(4)]
            send_ref[:part, k : k + wide] = slot[first]
            send_ref[part:, k : k + wide] = slot[3]
            own_ref[:, k : k + wide] = slot[0]
            pass_ref[:, k : k + wide] = slot[second]

    return pl.pallas_call(
        kernel,
        in_specs=[WHOLE] * 2,
        out_specs=[WHOLE] * 3,
        out_shape=[
            pltpu.VMEM((2 * part, half), bf16),
            pltpu.VMEM((part, half), bf16),
            pltpu.VMEM((part, half), bf16),
        ],
        cost_estimate=cost(2 * tokens * features * half, 2 * half * (tokens + features)),
        compiler_params=params(8 << 20),
        name="spread",
    )(proj_grad, query_weight)


def join(first, second):
    part, columns = first.shape

    def kernel(first_ref, second_ref, out_ref):
        out_ref[:part] = first_ref[...]
        out_ref[part:] = second_ref[...]

    return pl.pallas_call(
        kernel,
        in_specs=[WHOLE] * 2,
        out_specs=WHOLE,
        out_shape=pltpu.VMEM((2 * part, columns), bf16),
        cost_estimate=cost(1, 8 * part * columns),
        compiler_params=params(2 << 20),
        name="join",
    )(first, second)


def passed_on(kept, arrived):
    part, half = kept.shape

    def kernel(kept_ref, arrived_ref, out_ref):
        total = kept_ref[...].astype(f32) + arrived_ref[part:, :].astype(f32)
        out_ref[...] = total.astype(bf16)

    return pl.pallas_call(
        kernel,
        in_specs=[WHOLE] * 2,
        out_specs=WHOLE,
        out_shape=pltpu.VMEM((part, half), bf16),
        cost_estimate=cost(part * half, 6 * part * half),
        compiler_params=params(4 << 20),
        name="passed_on",
    )(kept, arrived)


def joined_total(halves):
    part, half = halves[0][0].shape

    def kernel(*refs):
        for color in range(2):
            own, one, two = refs[3 * color : 3 * color + 3]
            value = own[...].astype(f32) + one[:part, :].astype(f32) + two[...].astype(f32)
            refs[-1][:, color * half : (color + 1) * half] = value.astype(bf16)

    return pl.pallas_call(
        kernel,
        in_specs=[WHOLE] * 6,
        out_specs=WHOLE,
        out_shape=sds((part, 2 * half), bf16),
        cost_estimate=cost(4 * part * half, 10 * part * half),
        compiler_params=params(6 << 20),
        name="total",
    )(*halves[0], *halves[1])


def total_of(pieces):
    part, width = pieces[0].shape

    def kernel(*refs):
        refs[-1][...] = sum(ref[...].astype(f32) for ref in refs[:-1]).astype(bf16)

    return pl.pallas_call(
        kernel,
        in_specs=[WHOLE] * len(pieces),
        out_specs=WHOLE,
        out_shape=sds((part, width), bf16),
        cost_estimate=cost(4 * part * width, 10 * part * width),
        compiler_params=params(6 << 20),
        name="total",
    )(*pieces)


def add(kept, given):
    def kernel(kept_ref, given_ref, out_ref):
        out_ref[...] = kept_ref[...] + given_ref[...].astype(f32)

    if kept.shape[0] % 128:
        return kept + given.astype(f32)
    return pl.pallas_call(
        kernel,
        in_specs=[WHOLE] * 2,
        out_specs=WHOLE,
        out_shape=sds(kept.shape, f32),
        cost_estimate=cost(kept.size, 10 * kept.size),
        compiler_params=params(6 << 20),
        name="last",
    )(kept, given)


def weight_product(own, terms, grads, rows, cores, extra=(), dtype=f32):
    arrays = []
    for t in terms:
        if not any(t[0] is a for a in arrays):
            arrays.append(t[0])
    places = [next(i for i, a in enumerate(arrays) if a is t[0]) for t in terms]
    features = grads[0].shape[1]
    depth = sum(t[2] for t in terms)
    span = rows * cores if own is None else rows

    def first_column(core, start):
        if own is None:
            return start
        return start + (core if own else 1 - core) * rows

    def first_row(row, slot, part):
        return row if slot is None else (lax.axis_index("tensor") ^ slot) * part

    def kernel(*refs):
        core, plane = lax.axis_index("dp") % cores, lax.axis_index("dp") // cores
        xs, gs = refs[: len(arrays)], refs[len(arrays) : len(arrays) + len(grads)]
        out_ref, x_all, g_all = refs[-3], refs[-2], refs[-1]
        done = 0
        for place, (_, row, count, g, start, slot, planed) in zip(places, terms):
            offset = first_column(core, plane * rows * cores if planed else 0)
            cols = pl.ds(pl.multiple_of(offset, rows), span)
            begin = first_row(row, slot, count)
            x_all[done : done + count] = xs[place][pl.ds(pl.multiple_of(begin, count), count), cols]
            g_all[done : done + count] = gs[g][start : start + count]
            done += count
        value = dot(x_all[...], g_all[...], 0, 0)
        if extra:
            half = pl.ds(pl.multiple_of(first_column(core, 0), rows), span)
            value = value + refs[len(arrays) + len(grads)][half, :]
            for ref in refs[len(arrays) + len(grads) + 1 : -3]:
                value = value + ref[...].astype(f32)
        out_ref[...] = value.astype(dtype)

    if rows % 128:
        core, plane = lax.axis_index("dp") % cores, lax.axis_index("dp") // cores
        xs = [
            lax.dynamic_slice(
                t[0],
                (
                    first_row(t[1], t[5], t[2]),
                    first_column(core, plane * rows * cores if t[6] else 0),
                ),
                (t[2], span),
            )
            for t in terms
        ]
        gs = [grads[t[3]][t[4] : t[4] + t[2]] for t in terms]
        value = dot(jnp.concatenate(xs), jnp.concatenate(gs), 0, 0)
        if extra:
            value = value + lax.dynamic_slice_in_dim(extra[0], first_column(core, 0), span, 0)
            value = value + sum(e.astype(f32) for e in extra[1:])
        return value.astype(dtype)
    operands = arrays + list(grads) + list(extra)
    return pl.pallas_call(
        kernel,
        in_specs=[WHOLE] * len(operands),
        out_specs=WHOLE,
        out_shape=pltpu.VMEM((span, features), dtype),
        scratch_shapes=[pltpu.VMEM((depth, span), bf16), pltpu.VMEM((depth, features), bf16)],
        cost_estimate=cost(2 * span * features * depth, 4 * span * features),
        compiler_params=params(16 << 20),
        name="weight_product",
    )(*operands)


def make(mesh):
    dp, members = mesh.shape["dp"], mesh.shape["tensor"]
    cores = 2
    planes = dp // cores
    if dp % cores or planes & (planes - 1) or members & (members - 1):
        raise ValueError("sizes")

    def across(value, step):
        return lax.ppermute(value, "tensor", [(i, i ^ step) for i in range(members)])

    def along(value, step):
        pairs = [(i, i ^ (step * cores)) for i in range(dp)]
        return lax.ppermute(value, "dp", pairs)

    def per_device(block_input, query_weight, query_gain, query_grad):
        tokens, width = block_input.shape
        features = query_gain.shape[0]
        part = tokens // members
        columns = width // planes
        rows = columns // cores
        gain = query_gain.reshape(1, features)

        halved = False
        counts = [
            (s, (0,) if s > 1 else (0, 2) if halved else None) for s in range(planes - 1, 0, -1)
        ]
        held, blocks = stage(block_input, query_weight, query_grad, columns, part, counts, cores)
        block_input, query_weight, query_grad = held
        inputs = {s: along(block, s) for (s, _), block in zip(counts, blocks)}

        projected, sums = project(block_input, query_weight, query_grad, gain)
        step = 1
        while step < members // 2:
            sums = sums + across(sums, step)
            step *= 2
        sums = [sums, across(sums, step)] if members > 1 else [sums]
        proj_grad = backward(projected, query_grad, gain, sums, members)
        grads = {}
        for s in range(1, planes):
            low = s & -s
            grads[s] = along(proj_grad if s == low else grads[s - low], low)

        if members == 4:
            halves = []
            for color, (first, second) in enumerate(((1, 2), (2, 1))):
                send, own, kept = spread_half(proj_grad, query_weight, color, part)
                one = across(send, first)
                onward = passed_on(kept, one)
                halves.append((own, one, across(onward, second)))
            input_grad = joined_total(halves)
        else:
            pieces = spread(proj_grad, query_weight, members)
            pieces = [pieces[0]] + [across(pieces[r], r) for r in range(1, members)]
            input_grad = total_of(pieces)

        early = [(block_input, 0, part, 0, r * part, r, True) for r in range(members)]
        begun = weight_product(None, early, [proj_grad], rows, cores)
        late, order = [], list(grads)
        if halved and planes > 1:
            other = across(inputs[1], 1)
            for n, r in enumerate((0, 2)):
                late.append((inputs[1], n * part, part, 0, r * part, None, False))
                late.append((other, n * part, part, 0, (r ^ 1) * part, None, False))
        elif planes > 1:
            late += [(inputs[1], 0, part, 0, r * part, r, False) for r in range(members)]
        far = order[1:]
        late += [(inputs[s], 0, part, order.index(s), 0, None, False) for s in far]
        if members == 4 and len(far) <= 2:
            for s, (first, second) in zip(far, ((1, 2), (2, 1))):
                g = order.index(s)
                one = across(inputs[s], first)
                pair = join(inputs[s], one)
                two = across(pair, second)
                late += [
                    (one, 0, part, g, first * part, None, False),
                    (two, 0, part, g, second * part, None, False),
                    (two, part, part, g, 3 * part, None, False),
                ]
        elif far:
            joined = jnp.concatenate([inputs[s] for s in far])
            for r in range(1, members):
                array = across(joined, r)
                late += [
                    (array, k * part, part, order.index(s), r * part, None, False)
                    for k, s in enumerate(far)
                ]
        late_grads = [grads[s] for s in order]
        given = weight_product(0, late, late_grads, rows, cores, (begun,), bf16)
        given = lax.ppermute(given, "dp", [(i, i ^ 1) for i in range(dp)])
        kept = weight_product(1, late, late_grads, rows, cores, (begun,))
        weight_grad = add(kept, given)
        return (input_grad, weight_grad)

    return per_device


def solution(mesh):
    in_specs = (P("dp", None), P("tensor", None), P("tensor"), P("tensor", "dp"))
    out_specs = (P(("dp", "tensor"), None), P("dp", "tensor"))
    return jax.shard_map(
        make(mesh), mesh=mesh, in_specs=in_specs, out_specs=out_specs, check_vma=False
    )
```

```python
import jax
import jax.numpy as jnp
from jax import lax
from jax.experimental import pallas as pl
from jax.experimental.pallas import tpu as pltpu
from jax.sharding import PartitionSpec as P


epsilon = 1e-06
f32, bf16 = jnp.float32, jnp.bfloat16
WHOLE = pl.BlockSpec(memory_space=pltpu.VMEM)


def dot(a, b, ca, cb):
    return lax.dot_general(a, b, (((ca,), (cb,)), ((), ())), preferred_element_type=f32)


def cost(flops, nbytes):
    return pl.CostEstimate(flops=flops, bytes_accessed=nbytes, transcendentals=0)


def sds(shape, dtype):
    return jax.ShapeDtypeStruct(shape, dtype)


def chunk(size, most):
    fits = [c for c in range(128, most + 1, 128) if size % c == 0]
    return fits[-1] if fits else size


def params(nbytes):
    return pltpu.CompilerParams(vmem_limit_bytes=max(nbytes, 4 << 20))


def stage(block_input, columns, part, counts, cores):
    tokens = block_input.shape[0]
    shapes = [(tokens if slots is None else part * len(slots), columns) for _, slots in counts]

    def places(step, slots):
        plane, me = lax.axis_index("dp") // cores, lax.axis_index("tensor")
        rows = [(0, tokens)] if slots is None else [((me ^ r) * part, part) for r in slots]
        return [(row, count, (plane ^ step) * columns) for row, count in rows]

    if columns % 128:
        return [
            jnp.concatenate(
                [lax.dynamic_slice(block_input, (p[0], p[2]), (p[1], columns)) for p in places(*c)]
            )
            for c in counts
        ]

    def kernel(x_ref, *refs):
        *outs, sem = refs
        copies = []
        for out, entry in zip(outs, counts):
            done = 0
            for row, count, column in places(*entry):
                rows = pl.ds(pl.multiple_of(row, part), count)
                cols = pl.ds(pl.multiple_of(column, columns), columns)
                copies.append(
                    pltpu.make_async_copy(
                        x_ref.at[rows, cols], out.at[pl.ds(done, count)], sem.at[len(copies)]
                    )
                )
                copies[-1].start()
                done += count
        for copy in copies:
            copy.wait()

    pieces = sum(1 if slots is None else len(slots) for _, slots in counts)
    return pl.pallas_call(
        kernel,
        in_specs=[pl.BlockSpec(memory_space=pl.ANY)],
        out_specs=[WHOLE] * len(shapes),
        out_shape=[pltpu.VMEM(shape, bf16) for shape in shapes],
        scratch_shapes=[pltpu.SemaphoreType.DMA((pieces,))],
        cost_estimate=cost(10**10, 4 * sum(r * c for r, c in shapes)),
        compiler_params=params(2 << 20),
        name="stage",
    )(pltpu.with_memory_space_constraint(block_input, pltpu.HBM))


def column(row, size):
    return jnp.broadcast_to(row, (128, size)).T[:, :1]


def project(block_input, query_weight, query_grad, gain):
    tokens, width = block_input.shape
    features = query_weight.shape[0]
    wide = chunk(width, 2560)

    def kernel(x_ref, w_ref, g_ref, gain_ref, out_ref, sums_ref):
        for k in range(0, width, wide):
            product = dot(w_ref[:, k : k + wide], x_ref[:, k : k + wide], 1, 1)
            out_ref[...] = product if k == 0 else out_ref[...] + product
        projected = out_ref[...]
        scaled = g_ref[...].astype(f32) * column(gain_ref[...], features)
        sums_ref[0:1, :] = jnp.sum(projected * projected, axis=0, keepdims=True)
        sums_ref[1:2, :] = jnp.sum(scaled * projected, axis=0, keepdims=True)

    return pl.pallas_call(
        kernel,
        in_specs=[WHOLE] * 4,
        out_specs=[WHOLE] * 2,
        out_shape=[pltpu.VMEM((features, tokens), f32), pltpu.VMEM((2, tokens), f32)],
        cost_estimate=cost(2 * tokens * features * width, 2 * width * (tokens + features)),
        compiler_params=params(16 << 20),
        name="project",
    )(block_input, query_weight, query_grad, gain)


def backward(projected, query_grad, gain, sums, members):
    features, tokens = projected.shape
    part = tokens // members

    def kernel(p_ref, g_ref, gain_ref, *refs):
        *sums_refs, out_ref = refs
        total = sum(ref[...] for ref in sums_refs) / (features * members)
        inverse_rms = 1.0 / jnp.sqrt(total[0:1] + epsilon)
        coefficient = inverse_rms * inverse_rms * inverse_rms * total[1:2]
        scaled = g_ref[...].astype(f32) * column(gain_ref[...], features)
        grad = (inverse_rms * scaled - coefficient * p_ref[...]).T.astype(bf16)
        me = lax.axis_index("tensor")
        for q in range(members):
            rows = pl.ds(pl.multiple_of((me ^ q) * part, part), part)
            out_ref[rows, :] = grad[q * part : (q + 1) * part]

    return pl.pallas_call(
        kernel,
        in_specs=[WHOLE] * (3 + len(sums)),
        out_specs=WHOLE,
        out_shape=pltpu.VMEM((tokens, features), bf16),
        cost_estimate=cost(6 * features * tokens, 8 * features * tokens),
        compiler_params=params(6 << 20),
        name="backward",
    )(projected, query_grad, gain, *sums)


def spread(proj_grad, query_weight, members):
    tokens, features = proj_grad.shape
    width = query_weight.shape[1]
    part = tokens // members
    wide = chunk(width, 1280)

    def kernel(p_ref, w_ref, *outs):
        for k in range(0, width, wide):
            product = dot(p_ref[...], w_ref[:, k : k + wide], 1, 0).astype(bf16)
            for r in range(members):
                outs[r][:, k : k + wide] = product[r * part : (r + 1) * part]

    return pl.pallas_call(
        kernel,
        in_specs=[WHOLE] * 2,
        out_specs=[WHOLE] * members,
        out_shape=[sds((part, width), bf16)] * members,
        cost_estimate=cost(2 * tokens * features * width, 2 * width * (tokens + features)),
        compiler_params=params(8 << 20),
        name="spread",
    )(proj_grad, query_weight)


def spread_columns(proj_grad, query_weight, color, begin, end, part):
    tokens, features = proj_grad.shape
    half = end - begin
    first, second = (1, 2) if color == 0 else (2, 1)
    wide = chunk(half, 1280)

    def kernel(p_ref, w_ref, send_ref, own_ref, pass_ref):
        for k in range(0, half, wide):
            here = slice(begin + k, begin + k + wide)
            product = dot(p_ref[...], w_ref[:, here], 1, 0).astype(bf16)
            slot = [product[r * part : (r + 1) * part] for r in range(4)]
            send_ref[:part, k : k + wide] = slot[first]
            send_ref[part:, k : k + wide] = slot[3]
            own_ref[:, k : k + wide] = slot[0]
            pass_ref[:, k : k + wide] = slot[second]

    return pl.pallas_call(
        kernel,
        in_specs=[WHOLE] * 2,
        out_specs=[WHOLE] * 3,
        out_shape=[
            pltpu.VMEM((2 * part, half), bf16),
            pltpu.VMEM((part, half), bf16),
            pltpu.VMEM((part, half), bf16),
        ],
        cost_estimate=cost(2 * tokens * features * half, 2 * half * (tokens + features)),
        compiler_params=params(8 << 20),
        name="spread",
    )(proj_grad, query_weight)


def join(first, second):
    part, columns = first.shape

    def kernel(first_ref, second_ref, out_ref):
        out_ref[:part] = first_ref[...]
        out_ref[part:] = second_ref[...]

    return pl.pallas_call(
        kernel,
        in_specs=[WHOLE] * 2,
        out_specs=WHOLE,
        out_shape=pltpu.VMEM((2 * part, columns), bf16),
        cost_estimate=cost(1, 8 * part * columns),
        compiler_params=params(2 << 20),
        name="join",
    )(first, second)


def passed_on(kept, arrived):
    part, half = kept.shape

    def kernel(kept_ref, arrived_ref, out_ref):
        total = kept_ref[...].astype(f32) + arrived_ref[part:, :].astype(f32)
        out_ref[...] = total.astype(bf16)

    return pl.pallas_call(
        kernel,
        in_specs=[WHOLE] * 2,
        out_specs=WHOLE,
        out_shape=pltpu.VMEM((part, half), bf16),
        cost_estimate=cost(part * half, 6 * part * half),
        compiler_params=params(4 << 20),
        name="passed_on",
    )(kept, arrived)


def joined_total(halves):
    return jnp.concatenate(
        [
            (own.astype(f32) + one[: own.shape[0]].astype(f32) + two.astype(f32)).astype(bf16)
            for own, one, two in halves
        ],
        axis=1,
    )


def total_of(pieces):
    part, width = pieces[0].shape

    def kernel(*refs):
        refs[-1][...] = sum(ref[...].astype(f32) for ref in refs[:-1]).astype(bf16)

    return pl.pallas_call(
        kernel,
        in_specs=[WHOLE] * len(pieces),
        out_specs=WHOLE,
        out_shape=sds((part, width), bf16),
        cost_estimate=cost(4 * part * width, 10 * part * width),
        compiler_params=params(6 << 20),
        name="total",
    )(*pieces)


def finish(halves, kept, given):
    part, cut = halves[0][0].shape
    width = cut + halves[1][0].shape[1]
    rows, features = kept.shape
    steps = rows // 128

    def kernel(*refs):
        kept_ref, given_ref, input_hbm, weight_hbm, input_ref, weight_ref, sem = refs[6:]
        copies = []

        def leave(source, target):
            copies.append(pltpu.make_async_copy(source, target, sem.at[len(copies)]))
            copies[-1].start()

        for k in range(steps):
            here = slice(k * 128, (k + 1) * 128)
            weight_ref[here] = kept_ref[here] + given_ref[here].astype(f32)
            there = pl.ds(k * 128, 128)
            leave(weight_ref.at[there], weight_hbm.at[there])
        for color in range(2):
            own, one, two = refs[3 * color : 3 * color + 3]
            value = own[...].astype(f32) + one[:part, :].astype(f32) + two[...].astype(f32)
            begin, end = ((0, cut), (cut, width))[color]
            input_ref[:, begin:end] = value.astype(bf16)
            there = pl.ds(begin, end - begin)
            leave(input_ref.at[:, there], input_hbm.at[:, there])
        for copy in copies:
            copy.wait()

    return pl.pallas_call(
        kernel,
        in_specs=[WHOLE] * 8,
        out_specs=[pl.BlockSpec(memory_space=pl.ANY)] * 2,
        out_shape=[pltpu.HBM((part, width), bf16), pltpu.HBM((rows, features), f32)],
        scratch_shapes=[
            pltpu.VMEM((part, width), bf16),
            pltpu.VMEM((rows, features), f32),
            pltpu.SemaphoreType.DMA((steps + 2,)),
        ],
        cost_estimate=cost(kept.size, 10 * kept.size),
        compiler_params=params(8 << 20),
        name="finish",
    )(*halves[0], *halves[1], kept, given)


def weight_product(own, terms, grads, rows, cores, extra=(), dtype=f32):
    arrays = []
    for t in terms:
        if not any(t[0] is a for a in arrays):
            arrays.append(t[0])
    places = [next(i for i, a in enumerate(arrays) if a is t[0]) for t in terms]
    features = grads[0].shape[1]
    depth = sum(t[2] for t in terms)
    span = rows * cores if own is None else rows

    def first_column(core, start):
        if own is None:
            return start
        return start + (core if own else 1 - core) * rows

    def first_row(row, slot, part):
        return row if slot is None else (lax.axis_index("tensor") ^ slot) * part

    def kernel(*refs):
        core, plane = lax.axis_index("dp") % cores, lax.axis_index("dp") // cores
        xs, gs = refs[: len(arrays)], refs[len(arrays) : len(arrays) + len(grads)]
        out_ref, x_all, g_all = refs[-3], refs[-2], refs[-1]
        done = 0
        for place, (_, row, count, g, start, slot, planed) in zip(places, terms):
            offset = first_column(core, plane * rows * cores if planed else 0)
            cols = pl.ds(pl.multiple_of(offset, rows), span)
            begin = first_row(row, slot, count)
            x_all[done : done + count] = xs[place][pl.ds(pl.multiple_of(begin, count), count), cols]
            g_all[done : done + count] = gs[g][start : start + count]
            done += count
        value = dot(x_all[...], g_all[...], 0, 0)
        if extra:
            sofar = refs[len(arrays) + len(grads)]
            if own is None:
                value = value + sofar[...]
            else:
                value = value + sofar[pl.ds(pl.multiple_of(first_column(core, 0), rows), span), :]
            for ref in refs[len(arrays) + len(grads) + 1 : -3]:
                value = value + ref[...].astype(f32)
        out_ref[...] = value.astype(dtype)

    if rows % 128:
        core, plane = lax.axis_index("dp") % cores, lax.axis_index("dp") // cores
        xs = [
            lax.dynamic_slice(
                t[0],
                (
                    first_row(t[1], t[5], t[2]),
                    first_column(core, plane * rows * cores if t[6] else 0),
                ),
                (t[2], span),
            )
            for t in terms
        ]
        gs = [grads[t[3]][t[4] : t[4] + t[2]] for t in terms]
        value = dot(jnp.concatenate(xs), jnp.concatenate(gs), 0, 0)
        if extra:
            value = value + lax.dynamic_slice_in_dim(extra[0], first_column(core, 0), span, 0)
            value = value + sum(e.astype(f32) for e in extra[1:])
        return value.astype(dtype)
    operands = arrays + list(grads) + list(extra)
    return pl.pallas_call(
        kernel,
        in_specs=[WHOLE] * len(operands),
        out_specs=WHOLE,
        out_shape=pltpu.VMEM((span, features), dtype),
        scratch_shapes=[pltpu.VMEM((depth, span), bf16), pltpu.VMEM((depth, features), bf16)],
        cost_estimate=cost(2 * span * features * depth, 4 * span * features),
        compiler_params=params(16 << 20),
        name="weight_product",
    )(*operands)


def make(mesh):
    dp, members = mesh.shape["dp"], mesh.shape["tensor"]
    cores = 2
    planes = dp // cores
    if dp % cores or planes & (planes - 1) or members & (members - 1):
        raise ValueError("sizes")

    def across(value, step):
        return lax.ppermute(value, "tensor", [(i, i ^ step) for i in range(members)])

    def along(value, step):
        pairs = [(i, i ^ (step * cores)) for i in range(dp)]
        return lax.ppermute(value, "dp", pairs)

    def per_device(block_input, query_weight, query_gain, query_grad):
        tokens, width = block_input.shape
        features = query_gain.shape[0]
        part = tokens // members
        columns = width // planes
        rows = columns // cores
        gain = query_gain.reshape(1, features)

        counts = [(s, (0,) if s > 1 else None) for s in range(planes - 1, 0, -1)]
        blocks = stage(block_input, columns, part, counts, cores)
        inputs = {s: along(block, s) for (s, _), block in zip(counts, blocks)}

        projected, sums = project(block_input, query_weight, query_grad, gain)
        step = 1
        while step < members // 2:
            sums = sums + across(sums, step)
            step *= 2
        sums = [sums, across(sums, step)] if members > 1 else [sums]
        proj_grad = backward(projected, query_grad, gain, sums, members)
        grads = {}
        for s in range(1, planes):
            low = s & -s
            grads[s] = along(proj_grad if s == low else grads[s - low], low)

        if members == 4:
            halves = []
            cut = width * 1 // 2 // 128 * 128
            for color, (first, second) in enumerate(((1, 2), (2, 1))):
                begin, end = ((0, cut), (cut, width))[color]
                send, own, kept = spread_columns(proj_grad, query_weight, color, begin, end, part)
                one = across(send, first)
                onward = passed_on(kept, one)
                halves.append((own, one, across(onward, second)))
        else:
            pieces = spread(proj_grad, query_weight, members)
            pieces = [pieces[0]] + [across(pieces[r], r) for r in range(1, members)]
            input_grad = total_of(pieces)

        early = [(block_input, 0, part, 0, r * part, r, True) for r in range(members)]
        begun = weight_product(None, early, [proj_grad], rows, cores)
        order = list(grads)[1:]
        if planes > 1:
            near = [(inputs[1], 0, part, 0, r * part, r, False) for r in range(members)]
            begun = weight_product(None, near, [grads[1]], rows, cores, (begun,))
        late, far = [], order
        late += [(inputs[s], 0, part, order.index(s), 0, None, False) for s in far]
        if members == 4 and len(far) <= 2:
            for s, (first, second) in zip(far, ((1, 2), (2, 1))):
                g = order.index(s)
                one = across(inputs[s], first)
                pair = join(inputs[s], one)
                two = across(pair, second)
                late += [
                    (one, 0, part, g, first * part, None, False),
                    (two, 0, part, g, second * part, None, False),
                    (two, part, part, g, 3 * part, None, False),
                ]
        elif far:
            joined = jnp.concatenate([inputs[s] for s in far])
            for r in range(1, members):
                array = across(joined, r)
                late += [
                    (array, k * part, part, order.index(s), r * part, None, False)
                    for k, s in enumerate(far)
                ]
        if len(far) == 2:
            soon = [t[:3] + (0,) + t[4:] for t in late if t[3] == 0]
            late = [t[:3] + (0,) + t[4:] for t in late if t[3] == 1]
            begun = weight_product(None, soon, [grads[far[0]]], rows, cores, (begun,))
            order = order[1:]
        late_grads = [grads[s] for s in order]
        given = weight_product(0, late, late_grads, rows, cores, (begun,), bf16)
        given = lax.ppermute(given, "dp", [(i, i ^ 1) for i in range(dp)])
        kept = weight_product(1, late, late_grads, rows, cores, (begun,))
        if members == 4 and rows % 128 == 0:
            return tuple(finish(halves, kept, given))
        if members == 4:
            input_grad = joined_total(halves)
        return (input_grad, kept + given.astype(f32))

    return per_device


def solution(mesh):
    in_specs = (P("dp", None), P("tensor", None), P("tensor"), P("tensor", "dp"))
    out_specs = (P(("dp", "tensor"), None), P("dp", "tensor"))
    return jax.shard_map(
        make(mesh), mesh=mesh, in_specs=in_specs, out_specs=out_specs, check_vma=False
    )
```

```python
import jax
import jax.numpy as jnp
from jax import lax
from jax.experimental import pallas as pl
from jax.experimental.pallas import tpu as pltpu
from jax.sharding import PartitionSpec as P


epsilon = 1e-06
f32, bf16 = jnp.float32, jnp.bfloat16
WHOLE = pl.BlockSpec(memory_space=pltpu.VMEM)


def dot(a, b, ca, cb):
    return lax.dot_general(a, b, (((ca,), (cb,)), ((), ())), preferred_element_type=f32)


def cost(flops, nbytes):
    return pl.CostEstimate(flops=flops, bytes_accessed=nbytes, transcendentals=0)


def sds(shape, dtype):
    return jax.ShapeDtypeStruct(shape, dtype)


def chunk(size, most):
    fits = [c for c in range(128, most + 1, 128) if size % c == 0]
    return fits[-1] if fits else size


def params(nbytes):
    return pltpu.CompilerParams(vmem_limit_bytes=max(nbytes, 4 << 20))


def stage(block_input, columns, part, counts, cores):
    tokens = block_input.shape[0]
    shapes = [
        (tokens if slots is None else sum(count for _, count in slots), columns)
        for _, slots in counts
    ]

    def places(step, slots):
        plane, me = lax.axis_index("dp") // cores, lax.axis_index("tensor")
        rows = [(0, tokens)] if slots is None else [((me ^ r) * part, count) for r, count in slots]
        return [(row, count, (plane ^ step) * columns) for row, count in rows]

    if columns % 128:
        return [
            jnp.concatenate(
                [lax.dynamic_slice(block_input, (p[0], p[2]), (p[1], columns)) for p in places(*c)]
            )
            for c in counts
        ]

    def kernel(x_ref, *refs):
        *outs, sem = refs
        copies = []
        for out, entry in zip(outs, counts):
            done = 0
            for row, count, column in places(*entry):
                rows = pl.ds(pl.multiple_of(row, part), count)
                cols = pl.ds(pl.multiple_of(column, columns), columns)
                copies.append(
                    pltpu.make_async_copy(
                        x_ref.at[rows, cols], out.at[pl.ds(done, count)], sem.at[len(copies)]
                    )
                )
                copies[-1].start()
                done += count
        for copy in copies:
            copy.wait()

    pieces = sum(1 if slots is None else len(slots) for _, slots in counts)
    return pl.pallas_call(
        kernel,
        in_specs=[pl.BlockSpec(memory_space=pl.ANY)],
        out_specs=[WHOLE] * len(shapes),
        out_shape=[pltpu.VMEM(shape, bf16) for shape in shapes],
        scratch_shapes=[pltpu.SemaphoreType.DMA((pieces,))],
        cost_estimate=cost(10**10, 4 * sum(r * c for r, c in shapes)),
        compiler_params=params(2 << 20),
        name="stage",
    )(pltpu.with_memory_space_constraint(block_input, pltpu.HBM))


def column(row, size):
    return jnp.broadcast_to(row, (128, size)).T[:, :1]


def project(block_input, query_weight, query_grad, gain):
    tokens, width = block_input.shape
    features = query_weight.shape[0]
    wide = chunk(width, 2560)

    def kernel(x_ref, w_ref, g_ref, gain_ref, out_ref, sums_ref):
        for k in range(0, width, wide):
            product = dot(w_ref[:, k : k + wide], x_ref[:, k : k + wide], 1, 1)
            out_ref[...] = product if k == 0 else out_ref[...] + product
        projected = out_ref[...]
        scaled = g_ref[...].astype(f32) * column(gain_ref[...], features)
        sums_ref[0:1, :] = jnp.sum(projected * projected, axis=0, keepdims=True)
        sums_ref[1:2, :] = jnp.sum(scaled * projected, axis=0, keepdims=True)

    return pl.pallas_call(
        kernel,
        in_specs=[WHOLE] * 4,
        out_specs=[WHOLE] * 2,
        out_shape=[pltpu.VMEM((features, tokens), f32), pltpu.VMEM((2, tokens), f32)],
        cost_estimate=cost(2 * tokens * features * width, 2 * width * (tokens + features)),
        compiler_params=params(16 << 20),
        name="project",
    )(block_input, query_weight, query_grad, gain)


def backward(projected, query_grad, gain, sums, members):
    features, tokens = projected.shape
    part = tokens // members

    def kernel(p_ref, g_ref, gain_ref, *refs):
        *sums_refs, out_ref = refs
        total = sum(ref[...] for ref in sums_refs) / (features * members)
        inverse_rms = 1.0 / jnp.sqrt(total[0:1] + epsilon)
        coefficient = inverse_rms * inverse_rms * inverse_rms * total[1:2]
        scaled = g_ref[...].astype(f32) * column(gain_ref[...], features)
        grad = (inverse_rms * scaled - coefficient * p_ref[...]).T.astype(bf16)
        me = lax.axis_index("tensor")
        for q in range(members):
            rows = pl.ds(pl.multiple_of((me ^ q) * part, part), part)
            out_ref[rows, :] = grad[q * part : (q + 1) * part]

    return pl.pallas_call(
        kernel,
        in_specs=[WHOLE] * (3 + len(sums)),
        out_specs=WHOLE,
        out_shape=pltpu.VMEM((tokens, features), bf16),
        cost_estimate=cost(6 * features * tokens, 8 * features * tokens),
        compiler_params=params(6 << 20),
        name="backward",
    )(projected, query_grad, gain, *sums)


def spread(proj_grad, query_weight, members):
    tokens, features = proj_grad.shape
    width = query_weight.shape[1]
    part = tokens // members
    wide = chunk(width, 1280)

    def kernel(p_ref, w_ref, *outs):
        for k in range(0, width, wide):
            product = dot(p_ref[...], w_ref[:, k : k + wide], 1, 0).astype(bf16)
            for r in range(members):
                outs[r][:, k : k + wide] = product[r * part : (r + 1) * part]

    return pl.pallas_call(
        kernel,
        in_specs=[WHOLE] * 2,
        out_specs=[WHOLE] * members,
        out_shape=[sds((part, width), bf16)] * members,
        cost_estimate=cost(2 * tokens * features * width, 2 * width * (tokens + features)),
        compiler_params=params(8 << 20),
        name="spread",
    )(proj_grad, query_weight)


def spread_columns(proj_grad, query_weight, color, begin, end, part):
    tokens, features = proj_grad.shape
    half = end - begin
    first, second = (1, 2) if color == 0 else (2, 1)
    wide = chunk(half, 1280)

    def kernel(p_ref, w_ref, send_ref, own_ref, pass_ref):
        for k in range(0, half, wide):
            here = slice(begin + k, begin + k + wide)
            product = dot(p_ref[...], w_ref[:, here], 1, 0).astype(bf16)
            slot = [product[r * part : (r + 1) * part] for r in range(4)]
            send_ref[:part, k : k + wide] = slot[first]
            send_ref[part:, k : k + wide] = slot[3]
            own_ref[:, k : k + wide] = slot[0]
            pass_ref[:, k : k + wide] = slot[second]

    return pl.pallas_call(
        kernel,
        in_specs=[WHOLE] * 2,
        out_specs=[WHOLE] * 3,
        out_shape=[
            pltpu.VMEM((2 * part, half), bf16),
            pltpu.VMEM((part, half), bf16),
            pltpu.VMEM((part, half), bf16),
        ],
        cost_estimate=cost(2 * tokens * features * half, 2 * half * (tokens + features)),
        compiler_params=params(8 << 20),
        name="spread",
    )(proj_grad, query_weight)


def join(first, second):
    part, columns = first.shape

    def kernel(first_ref, second_ref, out_ref):
        out_ref[:part] = first_ref[...]
        out_ref[part:] = second_ref[...]

    return pl.pallas_call(
        kernel,
        in_specs=[WHOLE] * 2,
        out_specs=WHOLE,
        out_shape=pltpu.VMEM((2 * part, columns), bf16),
        cost_estimate=cost(1, 8 * part * columns),
        compiler_params=params(2 << 20),
        name="join",
    )(first, second)


def passed_on(kept, arrived):
    part, half = kept.shape

    def kernel(kept_ref, arrived_ref, out_ref):
        total = kept_ref[...].astype(f32) + arrived_ref[part:, :].astype(f32)
        out_ref[...] = total.astype(bf16)

    return pl.pallas_call(
        kernel,
        in_specs=[WHOLE] * 2,
        out_specs=WHOLE,
        out_shape=pltpu.VMEM((part, half), bf16),
        cost_estimate=cost(part * half, 6 * part * half),
        compiler_params=params(4 << 20),
        name="passed_on",
    )(kept, arrived)


def joined_total(halves):
    return jnp.concatenate(
        [
            (own.astype(f32) + one[: own.shape[0]].astype(f32) + two.astype(f32)).astype(bf16)
            for own, one, two in halves
        ],
        axis=1,
    )


def total_of(pieces):
    part, width = pieces[0].shape

    def kernel(*refs):
        refs[-1][...] = sum(ref[...].astype(f32) for ref in refs[:-1]).astype(bf16)

    return pl.pallas_call(
        kernel,
        in_specs=[WHOLE] * len(pieces),
        out_specs=WHOLE,
        out_shape=sds((part, width), bf16),
        cost_estimate=cost(4 * part * width, 10 * part * width),
        compiler_params=params(6 << 20),
        name="total",
    )(*pieces)


def finish(halves, kept, given):
    part, cut = halves[0][0].shape
    width = cut + halves[1][0].shape[1]
    rows, features = kept.shape
    steps = rows // 128

    def kernel(*refs):
        kept_ref, given_ref, input_hbm, weight_hbm, input_ref, weight_ref, sem = refs[6:]
        copies = []

        def leave(source, target):
            copies.append(pltpu.make_async_copy(source, target, sem.at[len(copies)]))
            copies[-1].start()

        for k in range(steps):
            here = slice(k * 128, (k + 1) * 128)
            weight_ref[here] = kept_ref[here] + given_ref[here].astype(f32)
            there = pl.ds(k * 128, 128)
            leave(weight_ref.at[there], weight_hbm.at[there])
        for color in range(2):
            own, one, two = refs[3 * color : 3 * color + 3]
            value = own[...].astype(f32) + one[:part, :].astype(f32) + two[...].astype(f32)
            begin, end = ((0, cut), (cut, width))[color]
            input_ref[:, begin:end] = value.astype(bf16)
            there = pl.ds(begin, end - begin)
            leave(input_ref.at[:, there], input_hbm.at[:, there])
        for copy in copies:
            copy.wait()

    return pl.pallas_call(
        kernel,
        in_specs=[WHOLE] * 8,
        out_specs=[pl.BlockSpec(memory_space=pl.ANY)] * 2,
        out_shape=[pltpu.HBM((part, width), bf16), pltpu.HBM((rows, features), f32)],
        scratch_shapes=[
            pltpu.VMEM((part, width), bf16),
            pltpu.VMEM((rows, features), f32),
            pltpu.SemaphoreType.DMA((steps + 2,)),
        ],
        cost_estimate=cost(kept.size, 10 * kept.size),
        compiler_params=params(8 << 20),
        name="finish",
    )(*halves[0], *halves[1], kept, given)


def weight_product(own, terms, grads, rows, cores, extra=(), dtype=f32):
    arrays = []
    for t in terms:
        if not any(t[0] is a for a in arrays):
            arrays.append(t[0])
    places = [next(i for i, a in enumerate(arrays) if a is t[0]) for t in terms]
    features = grads[0].shape[1]
    depth = sum(t[2] for t in terms)
    span = rows * cores if own is None else rows

    def first_column(core, start):
        if own is None:
            return start
        return start + (core if own else 1 - core) * rows

    def first_row(row, slot, part):
        return row if slot is None else (lax.axis_index("tensor") ^ slot) * part

    def kernel(*refs):
        core, plane = lax.axis_index("dp") % cores, lax.axis_index("dp") // cores
        xs, gs = refs[: len(arrays)], refs[len(arrays) : len(arrays) + len(grads)]
        out_ref, x_all, g_all = refs[-3], refs[-2], refs[-1]
        done = 0
        for place, (_, row, count, g, start, slot, planed) in zip(places, terms):
            offset = first_column(core, plane * rows * cores if planed else 0)
            cols = pl.ds(pl.multiple_of(offset, rows), span)
            begin = row if slot is None else pl.multiple_of(first_row(row, slot, count), count)
            x_all[done : done + count] = xs[place][pl.ds(begin, count), cols]
            g_all[done : done + count] = gs[g][start : start + count]
            done += count
        value = dot(x_all[...], g_all[...], 0, 0)
        if extra:
            sofar = refs[len(arrays) + len(grads)]
            if own is None:
                value = value + sofar[...]
            else:
                value = value + sofar[pl.ds(pl.multiple_of(first_column(core, 0), rows), span), :]
            for ref in refs[len(arrays) + len(grads) + 1 : -3]:
                value = value + ref[...].astype(f32)
        out_ref[...] = value.astype(dtype)

    if rows % 128:
        core, plane = lax.axis_index("dp") % cores, lax.axis_index("dp") // cores
        xs = [
            lax.dynamic_slice(
                t[0],
                (
                    first_row(t[1], t[5], t[2]),
                    first_column(core, plane * rows * cores if t[6] else 0),
                ),
                (t[2], span),
            )
            for t in terms
        ]
        gs = [grads[t[3]][t[4] : t[4] + t[2]] for t in terms]
        value = dot(jnp.concatenate(xs), jnp.concatenate(gs), 0, 0)
        if extra:
            value = value + lax.dynamic_slice_in_dim(extra[0], first_column(core, 0), span, 0)
            value = value + sum(e.astype(f32) for e in extra[1:])
        return value.astype(dtype)
    operands = arrays + list(grads) + list(extra)
    return pl.pallas_call(
        kernel,
        in_specs=[WHOLE] * len(operands),
        out_specs=WHOLE,
        out_shape=pltpu.VMEM((span, features), dtype),
        scratch_shapes=[pltpu.VMEM((depth, span), bf16), pltpu.VMEM((depth, features), bf16)],
        cost_estimate=cost(2 * span * features * depth, 4 * span * features),
        compiler_params=params(16 << 20),
        name="weight_product",
    )(*operands)


def make(mesh):
    dp, members = mesh.shape["dp"], mesh.shape["tensor"]
    cores = 2
    planes = dp // cores
    if dp % cores or planes & (planes - 1) or members & (members - 1):
        raise ValueError("sizes")

    def across(value, step):
        return lax.ppermute(value, "tensor", [(i, i ^ step) for i in range(members)])

    def along(value, step):
        pairs = [(i, i ^ (step * cores)) for i in range(dp)]
        return lax.ppermute(value, "dp", pairs)

    def per_device(block_input, query_weight, query_gain, query_grad):
        tokens, width = block_input.shape
        features = query_gain.shape[0]
        part = tokens // members
        columns = width // planes
        rows = columns // cores
        gain = query_gain.reshape(1, features)

        lent = 32 if members == 4 and part % 64 == 0 else 0
        most = ((0, part), (1, part - lent), (2, part), (3, part)) if lent else None
        counts = [(s, ((0, part),) if s > 1 else most) for s in range(planes - 1, 0, -1)]
        blocks = stage(block_input, columns, part, counts, cores)
        inputs = {s: along(block, s) for (s, _), block in zip(counts, blocks)}

        projected, sums = project(block_input, query_weight, query_grad, gain)
        step = 1
        while step < members // 2:
            sums = sums + across(sums, step)
            step *= 2
        sums = [sums, across(sums, step)] if members > 1 else [sums]
        proj_grad = backward(projected, query_grad, gain, sums, members)
        grads = {}
        for s in range(1, planes):
            low = s & -s
            grads[s] = along(proj_grad if s == low else grads[s - low], low)

        if members == 4:
            halves = []
            cut = width * 1 // 2 // 128 * 128
            for color, (first, second) in enumerate(((1, 2), (2, 1))):
                begin, end = ((0, cut), (cut, width))[color]
                send, own, kept = spread_columns(proj_grad, query_weight, color, begin, end, part)
                one = across(send, first)
                onward = passed_on(kept, one)
                halves.append((own, one, across(onward, second)))
        else:
            pieces = spread(proj_grad, query_weight, members)
            pieces = [pieces[0]] + [across(pieces[r], r) for r in range(1, members)]
            input_grad = total_of(pieces)

        early = [(block_input, 0, part, 0, r * part, r, True) for r in range(members)]
        begun = weight_product(None, early, [proj_grad], rows, cores)
        order = list(grads)[1:]
        if planes > 1:
            near = [(inputs[1], 0, part, 0, r * part, r, False) for r in range(members)]
            if lent:
                borrowed = across(inputs[1][part - lent : part], 1)
                near = [
                    (inputs[1], 0, 2 * part - lent, 0, 0, None, False),
                    (inputs[1], 2 * part - lent, 2 * part, 0, 2 * part, None, False),
                ]
            begun = weight_product(None, near, [grads[1]], rows, cores, (begun,))
        late, far = [], order
        late += [(inputs[s], 0, part, order.index(s), 0, None, False) for s in far]
        if members == 4 and len(far) <= 2:
            for s, (first, second) in zip(far, ((2, 1), (1, 2))):
                g = order.index(s)
                one = across(inputs[s], first)
                pair = join(inputs[s], one)
                two = across(pair, second)
                late += [
                    (one, 0, part, g, first * part, None, False),
                    (two, 0, part, g, second * part, None, False),
                    (two, part, part, g, 3 * part, None, False),
                ]
        elif far:
            joined = jnp.concatenate([inputs[s] for s in far])
            for r in range(1, members):
                array = across(joined, r)
                late += [
                    (array, k * part, part, order.index(s), r * part, None, False)
                    for k, s in enumerate(far)
                ]
        if len(far) == 2:
            soon = [t[:3] + (0,) + t[4:] for t in late if t[3] == 0]
            late = [t[:3] + (0,) + t[4:] for t in late if t[3] == 1]
            begun = weight_product(None, soon, [grads[far[0]]], rows, cores, (begun,))
            order = order[1:]
        late_grads = [grads[s] for s in order]
        if lent:
            late.append((borrowed, 0, lent, len(order), 2 * part - lent, None, False))
            late_grads.append(grads[1])
        given = weight_product(0, late, late_grads, rows, cores, (begun,), bf16)
        given = lax.ppermute(given, "dp", [(i, i ^ 1) for i in range(dp)])
        kept = weight_product(1, late, late_grads, rows, cores, (begun,))
        if members == 4 and rows % 128 == 0:
            return tuple(finish(halves, kept, given))
        if members == 4:
            input_grad = joined_total(halves)
        return (input_grad, kept + given.astype(f32))

    return per_device


def solution(mesh):
    in_specs = (P("dp", None), P("tensor", None), P("tensor"), P("tensor", "dp"))
    out_specs = (P(("dp", "tensor"), None), P("dp", "tensor"))
    return jax.shard_map(
        make(mesh), mesh=mesh, in_specs=in_specs, out_specs=out_specs, check_vma=False
    )
```
